32 devices in a mesh: rep: 1, r: 8 (over y, z), s: 4 (over x, core).
Axes of the slice: x: 2, y: 2, z: 4, core: 2. Of those that a mesh axis runs over, the one named last changes fastest.
Arguments:
- x: bfloat16 [32, 4096, 640], P(('rep', 'r', 's'))
- dy: bfloat16 [32, 4096, 640], P(('rep', 'r', 's'))
- w_gate: bfloat16 [2, 640, 2048], P(None, 's')
- w_up: bfloat16 [2, 640, 2048], P(None, 's')
- w_down: bfloat16 [2, 2048, 640], P(None, 's')
Outputs:
- output 1: bfloat16 [32, 4096, 640], P(('rep', 'r', 's'))
- output 2: bfloat16 [2, 640, 2048], P('rep', 's')
- output 3: bfloat16 [2, 640, 2048], P('rep', 's')
- output 4: bfloat16 [2, 2048, 640], P('rep', 's')
All inputs are finite; a program needn't handle non-finite values.
Results may differ from the reference program's by a relative error of at most 0.018.
Values are sent between devices in bfloat16 or wider.
A program may use at most 2 GiB of HBM per device.

```python
import jax
import jax.numpy as jnp
from jax import lax

SEQUENCES = 32
TOKENS = 4096
D = 640
FF = 2048
LAYERS = 2
NAMES = ("w_gate", "w_up", "w_down")
SHAPES = {"w_gate": (LAYERS, D, FF), "w_up": (LAYERS, D, FF), "w_down": (LAYERS, FF, D)}


def bump(key, n, height):
    away = (jnp.arange(n, dtype=jnp.int32) - jax.random.randint(key, (), 0, n, jnp.int32)) % n
    return jnp.where(away < n // 8, height, 1.0)


def together(key, own, strength):
    shared = jax.random.normal(key, own.shape[1:], jnp.float32)
    return (own + strength * shared) * lax.rsqrt(1 + strength * strength)


def setup_inputs(seed: int = 0, part: int = 0) -> dict:
    kx, kdy, ka, kb, kz, kf, kh, kl, *kw = jax.random.split(jax.random.key(seed), 8 + len(NAMES))
    kx, kdy, ka, kb = (jax.random.fold_in(k, part) for k in (kx, kdy, ka, kb))
    shape = (SEQUENCES, TOKENS, D)
    much_x, much_dy = jax.random.uniform(kz, (2,), jnp.float32, 0.0, 1.0)
    layers = 2.0 ** jax.random.uniform(kl, (LAYERS, 1, 1), jnp.float32, -1.0, 1.0)
    x = together(ka, jax.random.normal(kx, shape, jnp.float32), much_x) * bump(kf, D, 4.0)
    dy = together(kb, jax.random.normal(kdy, shape, jnp.float32), much_dy)
    drawn = {"x": x.astype(jnp.bfloat16), "dy": (dy * (SEQUENCES * TOKENS) ** -0.5).astype(jnp.bfloat16)}
    for key, name in zip(kw, NAMES, strict=True):
        w = jax.random.normal(key, SHAPES[name], jnp.float32) * SHAPES[name][1] ** -0.5
        drawn[name] = (w * {"w_gate": 1.0, "w_up": bump(kh, FF, 4.0), "w_down": layers}[name]).astype(jnp.bfloat16)
    return drawn


def matmul(a, w):
    return jnp.dot(a, w, preferred_element_type=jnp.float32).astype(jnp.bfloat16)


def normed(h):
    wide = h.astype(jnp.float32)
    scale = lax.rsqrt(jnp.mean(wide**2, -1, keepdims=True) + 1e-6)
    return (wide * scale).astype(jnp.bfloat16)


def layer(h, w):
    a = normed(h)
    gate = jnp.dot(a, w["w_gate"], preferred_element_type=jnp.float32)
    up = jnp.dot(a, w["w_up"], preferred_element_type=jnp.float32)
    return h + matmul((jax.nn.silu(gate) * up).astype(jnp.bfloat16), w["w_down"])


def stack(weights, h):
    return lax.scan(lambda h, w: (layer(h, w), None), h, weights)[0]


def reference(x, dy, w_gate, w_up, w_down):
    weights = dict(zip(NAMES, (w_gate, w_up, w_down), strict=True))

    def take(so_far, sequence):
        h, by_y = sequence
        _, back = jax.vjp(stack, weights, h)
        by_weights, by_h = back(by_y)
        return jax.tree.map(lambda total, term: total + term.astype(jnp.float32), so_far, by_weights), by_h

    none_yet = {name: jnp.zeros(w.shape, jnp.float32) for name, w in weights.items()}
    by_weights, by_x = lax.scan(take, none_yet, (x, dy))
    return (by_x, *(by_weights[name].astype(jnp.bfloat16) for name in NAMES))
```

```python
import jax
import jax.numpy as jnp
from jax import lax
from jax.experimental import pallas as pl
from jax.experimental.pallas import tpu as pltpu
from jax.sharding import PartitionSpec as P

T, D, F = 4096, 640, 2048
TB, FC = 512, 512
NB, J = T // TB, F // FC
STEPS = NB * J
XS, CS, YS, ZS = 2, 2, 2, 4
HR, QL = D // 8, FC // 4
SLOTS = 6
TICKS = 46
VMEM_LIMIT = 67_000_000
bf16, f32 = jnp.bfloat16, jnp.float32
NT = (((1,), (1,)), ((), ()))
MESH = pl.DeviceIdType.MESH


def dot(a, b):
    return jnp.dot(a, b, preferred_element_type=f32)


def dot_nt(a, b):
    return lax.dot_general(a, b, NT, preferred_element_type=f32)


def scale_of(wide):
    return lax.rsqrt(jnp.mean(wide * wide, -1, keepdims=True) + 1e-6)


def fwd_kernel(h_hbm, wg_hbm, wu_hbm, wd_hbm, o_hbm, h_v, a_v, yT_v, wg_v, wu_v, wd_v, wdT_v, s_v, sem, osem):
    copies = [
        pltpu.make_async_copy(src, dst, sem.at[i])
        for i, (src, dst) in enumerate([(h_hbm, h_v), (wg_hbm, wg_v), (wu_hbm, wu_v), (wd_hbm, wd_v)])
    ]
    for copy in copies:
        copy.start()
    yT_v[...] = jnp.zeros_like(yT_v)
    s_v[1] = jnp.zeros_like(s_v[1])
    copies[0].wait()

    @pl.loop(0, NB)
    def _(t):
        wide = h_v[t].astype(f32)
        a_v[t] = (wide * scale_of(wide)).astype(bf16)

    for copy in copies[1:]:
        copy.wait()

    @pl.loop(0, J)
    def _(j):
        wdT_v[j] = wd_v[j].T

    def front(j, t):
        return dot(a_v[t], wg_v[j]), dot(a_v[t], wu_v[j])

    def mid(gate, up):
        return (gate * jax.nn.sigmoid(gate) * up).astype(bf16)

    def back(j, t, act):
        yT_v[t] += dot_nt(wdT_v[j], act)

    @pl.loop(0, STEPS // 2)
    def _(pair):
        i = 2 * pair
        before = jnp.maximum(i - 1, 0)
        first = front(i // NB, i % NB)
        back(before // NB, before % NB, s_v[1])
        s_v[0] = mid(*first)
        second = front((i + 1) // NB, (i + 1) % NB)
        back(i // NB, i % NB, s_v[0])
        s_v[1] = mid(*second)

    back(J - 1, NB - 1, s_v[1])

    @pl.loop(0, NB)
    def _(t):
        h_v[t] = h_v[t] + yT_v[t].astype(bf16).T

    copy = pltpu.make_async_copy(h_v, o_hbm, osem)
    copy.start()
    copy.wait()


def forward(h, wg, wu, wd):
    anywhere = pl.BlockSpec(memory_space=pl.ANY)
    return pl.pallas_call(
        fwd_kernel,
        out_shape=jax.ShapeDtypeStruct((NB, TB, D), bf16),
        in_specs=[anywhere] * 4,
        out_specs=anywhere,
        scratch_shapes=[
            pltpu.VMEM((NB, TB, D), bf16),
            pltpu.VMEM((NB, TB, D), bf16),
            pltpu.VMEM((NB, D, TB), f32),
            pltpu.VMEM((J, D, FC), bf16),
            pltpu.VMEM((J, D, FC), bf16),
            pltpu.VMEM((J, FC, D), bf16),
            pltpu.VMEM((J, D, FC), bf16),
            pltpu.VMEM((2, TB, FC), bf16),
            pltpu.SemaphoreType.DMA((4,)),
            pltpu.SemaphoreType.DMA,
        ],
        compiler_params=pltpu.CompilerParams(vmem_limit_bytes=VMEM_LIMIT),
        cost_estimate=pl.CostEstimate(flops=6 * T * D * F, bytes_accessed=20_000_000, transcendentals=0),
        name="forward",
    )(h, wg, wu, wd)


class Reduction:
    def __init__(self, g1_hbm, g0_hbm, out_hbm, gbuf, drecv, xs, xrecv, ys, yrecv, keep, zs, zrecv, fq, dsem, xsem, ysem, zsem, fsem, asem, lsem, psem, near):
        self.__dict__.update({k: v for k, v in locals().items() if k != "self"})
        r, s = lax.axis_index("r"), lax.axis_index("s")
        self.y, self.z, self.x, self.c = r // ZS, r % ZS, s // CS, s % CS
        self.partner = {"s": self.x * CS + 1 - self.c}
        self.xpeer = {"s": (1 - self.x) * CS + self.c}
        self.ypeer = {"r": (1 - self.y) * ZS + self.z}
        self.zpeers = [{"r": self.y * ZS + (self.z + d) % ZS} for d in range(1, ZS)]
        self.peers = [self.partner, self.xpeer, self.ypeer, *self.zpeers]

    def enter(self):
        barrier = pltpu.get_barrier_semaphore()
        for peer in self.peers:
            pl.semaphore_signal(barrier, inc=1, device_id=peer, device_id_type=MESH)
        pl.semaphore_wait(barrier, len(self.peers))

    def load(self, g):
        return pltpu.make_async_copy(self.g1_hbm.at[g], self.gbuf.at[g % 2], self.psem)

    def load0(self, g):
        return pltpu.make_async_copy(self.g0_hbm.at[g - J], self.gbuf.at[g % 2], self.psem)

    def at(self, k):
        block = k // 4
        return (k >= 0) & (k % 4 < 3) & (block != 6) & (block < 9), block - jnp.where(block > 6, 1, 0), k % 4

    def remote(self, src, dst, sems, peer):
        return pltpu.make_async_remote_copy(src, dst, sems.at[0], sems.at[1], device_id=peer, device_id_type=MESH)

    def dcopy(self, b, m, slot):
        return self.remote(self.gbuf.at[b, m, 1 - self.c], self.drecv.at[slot], self.dsem.at[slot], self.partner)

    def xcopy(self, slot):
        return self.remote(self.xs.at[slot], self.xrecv.at[slot], self.xsem.at[slot], self.xpeer)

    def ycopy(self, slot):
        return self.remote(self.ys.at[slot], self.yrecv.at[slot], self.ysem.at[slot], self.ypeer)

    def zcopies(self, slot):
        return [self.remote(self.zs.at[slot, i], self.zrecv.at[slot, i], self.zsem.at[slot, i], peer) for i, peer in enumerate(self.zpeers)]

    def fcopies(self, g, m, slot):
        place = self.out_hbm.at[g, m, self.y, self.z]
        return [self.remote(self.fq.at[slot], place, self.fsem.at[slot, i], peer) for i, peer in enumerate(self.zpeers)] + [
            pltpu.make_async_copy(self.fq.at[slot], place, self.lsem.at[slot])
        ]

    def acopy(self, g, m, slot):
        half = self.out_hbm.at[g, m, self.y]
        return self.remote(half, half, self.asem.at[slot], self.ypeer)

    def stage(self, k, delay, body):
        valid, g, m = self.at(k - delay)

        @pl.when(valid)
        def _():
            body(g, m, (k - delay) % SLOTS)

    def tick(self, k):
        x, c, y, z = self.x, self.c, self.y, self.z
        gbuf, drecv, xrecv, keep = self.gbuf, self.drecv, self.xrecv, self.keep

        @pl.when(k >= 2)
        def _():
            for i in range(len(self.peers)):
                pl.semaphore_wait(self.near.at[i], 1)

        ahead = k + 2
        block = ahead // 4
        turn = (ahead % 4 == 0) & (k >= 0)

        @pl.when(turn & (block < J))
        def _():
            self.load(block).start()

        @pl.when(turn & (block >= J) & (block < 8) & (block != 6))
        def _():
            self.load0(block - jnp.where(block > 6, 1, 0)).start()

        def end(g, m, slot):
            self.acopy(g, m, slot).wait()

        def gather_y(g, m, slot):
            for copy in self.fcopies(g, m, slot):
                copy.wait()
            self.acopy(g, m, slot).start()

        def finish(g, m, slot):
            for copy in self.zcopies(slot):
                copy.wait()
            total = keep[slot, z]
            for i in range(ZS - 1):
                total += self.zrecv[slot, i].astype(f32)
            self.fq[slot] = total.astype(bf16)
            for copy in self.fcopies(g, m, slot):
                copy.start()

        def to_z(g, m, slot):
            self.ycopy(slot).wait()
            keep[slot] += self.yrecv[slot].astype(f32)
            for i in range(ZS - 1):
                self.zs[slot, i] = keep[slot, (z + i + 1) % ZS].astype(bf16)
            for copy in self.zcopies(slot):
                copy.start()

        def to_y(g, m, slot):
            self.xcopy(slot).wait()

            def total(half):
                return gbuf[g % 2, m, c, x, half].astype(f32) + drecv[slot, x, half].astype(f32) + xrecv[slot, half].astype(f32)

            self.ys[slot] = total(1 - y).astype(bf16)
            self.ycopy(slot).start()
            keep[slot] = total(y)

        def to_x(g, m, slot):
            self.dcopy(g % 2, m, slot).wait()
            self.xs[slot] = (gbuf[g % 2, m, c, 1 - x].astype(f32) + drecv[slot, 1 - x].astype(f32)).astype(bf16)
            self.xcopy(slot).start()

        def to_partner(g, m, slot):
            @pl.when((m == 0) & (g < J))
            def _():
                self.load(g).wait()

            @pl.when((m == 0) & (g >= J) & (g < 2 * J - 1))
            def _():
                self.load0(g).wait()

            self.dcopy(g % 2, m, slot).start()

        self.stage(k, 11, end)
        self.stage(k, 9, gather_y)
        self.stage(k, 7, finish)
        self.stage(k, 5, to_z)
        self.stage(k, 3, to_y)
        self.stage(k, 1, to_x)
        self.stage(k, 0, to_partner)

        @pl.when(k < TICKS - 2)
        def _():
            for i, peer in enumerate(self.peers):
                pl.semaphore_signal(self.near.at[i], inc=1, device_id=peer, device_id_type=MESH)


def bwd_kernel(reduce, *refs):
    h_hbm, dy_hbm, wg_hbm, wu_hbm, wd_hbm, *refs = refs
    g1_hbm, dh_hbm, g_hbm, *refs = refs if reduce else (None, *refs)
    out_hbm, *refs = refs if reduce else (None, *refs)
    dy_v, a_v, aT_v, dyT_v, daT_v, wg_v, wu_v, wd_v, acc_v, gb_v, s_v, sem, gsem, hsem, *refs = refs
    copies = [
        pltpu.make_async_copy(src, dst, sem.at[i])
        for i, (src, dst) in enumerate([(h_hbm, a_v), (dy_hbm, dy_v), (wg_hbm, wg_v), (wu_hbm, wu_v), (wd_hbm, wd_v)])
    ]
    for copy in copies:
        copy.start()
    red = None
    if reduce:
        red = Reduction(g1_hbm, g_hbm, out_hbm, *refs)
        red.load(0).start()
        red.enter()
    acc_v[...] = jnp.zeros_like(acc_v)
    daT_v[...] = jnp.zeros_like(daT_v)
    s_v[1] = jnp.zeros_like(s_v[1])
    copies[0].wait()
    copies[1].wait()

    @pl.loop(0, NB)
    def _(t):
        wide = a_v[t].astype(f32)
        a = (wide * scale_of(wide)).astype(bf16)
        a_v[t] = a
        aT_v[t] = a.T
        dyT_v[t] = dy_v[t].T

    for copy in copies[2:]:
        copy.wait()

    def front(j, t):
        return dot(a_v[t], wg_v[j]), dot(a_v[t], wu_v[j]), dot_nt(dy_v[t], wd_v[j])

    def mid(slot, gate, up, dact):
        dact = dact.astype(bf16).astype(f32)
        sg = jax.nn.sigmoid(gate)
        s = gate * sg
        s_v[slot, 0] = (s * up).astype(bf16)
        s_v[slot, 1] = (dact * up * (sg + s * (1.0 - sg))).astype(bf16)
        s_v[slot, 2] = (dact * s).astype(bf16)

    def back(j, t, slot):
        act, dgate, dup = s_v[slot, 0], s_v[slot, 1], s_v[slot, 2]
        daT_v[t] += dot_nt(wg_v[j], dgate) + dot_nt(wu_v[j], dup)
        acc_v[0] += dot(aT_v[t], dgate)
        acc_v[1] += dot(aT_v[t], dup)
        acc_v[2] += dot(dyT_v[t], act)

    def flush(dst):
        for x in range(XS):
            for c in range(CS):
                n = x * CS + c
                for h in range(2):
                    for q in range(4):
                        rows = slice(n * 2 * HR + h * HR, n * 2 * HR + (h + 1) * HR)
                        for m in range(2):
                            dst[m, c, x, h, q] = acc_v[m, rows, q * QL : (q + 1) * QL].astype(bf16)
                        rows = slice(q * 2 * HR + h * HR, q * 2 * HR + (h + 1) * HR)
                        dst[2, c, x, h, q] = acc_v[2, rows, n * QL : (n + 1) * QL].astype(bf16)

    def put(j):
        return pltpu.make_async_copy(gb_v, g_hbm.at[j], gsem)

    @pl.loop(0, STEPS // 2)
    def _(pair):
        i = 2 * pair
        before = jnp.maximum(i - 1, 0)
        first = front(i // NB, i % NB)
        back(before // NB, before % NB, 1)
        mid(0, *first)

        @pl.when((i % NB == 0) & (pair > 0))
        def _():
            flush(gb_v)
            put(before // NB).start()
            acc_v[...] = jnp.zeros_like(acc_v)

        if reduce:
            red.tick(i)
        second = front((i + 1) // NB, (i + 1) % NB)
        back(i // NB, i % NB, 0)
        mid(1, *second)

        @pl.when((i % NB == 0) & (pair > 0))
        def _():
            put(before // NB).wait()

        if reduce:
            red.tick(i + 1)

    reload = pltpu.make_async_copy(h_hbm, a_v, hsem)
    reload.start()
    back(J - 1, NB - 1, 1)
    if reduce:
        flush(red.gbuf.at[1])
    else:
        flush(gb_v)
        put(J - 1).start()
    reload.wait()

    @pl.loop(0, NB)
    def _(t):
        if reduce:
            red.tick(STEPS + t)
        da = daT_v[t].astype(bf16).T.astype(f32)
        wide = a_v[t].astype(f32)
        scale = scale_of(wide)
        mean = jnp.mean(da * wide, -1, keepdims=True)
        dy_v[t] = dy_v[t] + (da * scale - wide * (scale * scale * scale * mean)).astype(bf16)

    copy = pltpu.make_async_copy(dy_v, dh_hbm, hsem)
    copy.start()
    if reduce:

        @pl.loop(STEPS + NB, TICKS)
        def _(k):
            red.tick(k)

    else:
        put(J - 1).wait()
    copy.wait()


def backward(h, dy, wg, wu, wd, g1=None):
    reduce = g1 is not None
    anywhere = pl.BlockSpec(memory_space=pl.ANY)
    tokens, turned, grads = (NB, TB, D), (NB, D, TB), (J, 3, CS, XS, 2, 4, HR, QL)
    outs = [jax.ShapeDtypeStruct(tokens, bf16), jax.ShapeDtypeStruct(grads, bf16)]
    scratch = [
        pltpu.VMEM(tokens, bf16),
        pltpu.VMEM(tokens, bf16),
        pltpu.VMEM(turned, bf16),
        pltpu.VMEM(turned, bf16),
        pltpu.VMEM(turned, f32),
        pltpu.VMEM((J, D, FC), bf16),
        pltpu.VMEM((J, D, FC), bf16),
        pltpu.VMEM((J, FC, D), bf16),
        pltpu.VMEM((3, D, FC), f32),
        pltpu.VMEM(grads[1:], bf16),
        pltpu.VMEM((2, 3, TB, FC), bf16),
        pltpu.SemaphoreType.DMA((5,)),
        pltpu.SemaphoreType.DMA,
        pltpu.SemaphoreType.DMA,
    ]
    if reduce:
        piece = (2, 4, HR, QL)
        outs.append(jax.ShapeDtypeStruct((2 * J, 3, *piece), bf16))
        pair = pltpu.SemaphoreType.DMA((SLOTS, 2))
        triple = pltpu.SemaphoreType.DMA((SLOTS, ZS - 1, 2))
        scratch += [
            pltpu.VMEM((2, *grads[1:]), bf16),
            pltpu.VMEM((SLOTS, XS, *piece), bf16),
            pltpu.VMEM((SLOTS, *piece), bf16),
            pltpu.VMEM((SLOTS, *piece), bf16),
            pltpu.VMEM((SLOTS, *piece[1:]), bf16),
            pltpu.VMEM((SLOTS, *piece[1:]), bf16),
            pltpu.VMEM((SLOTS, *piece[1:]), f32),
            pltpu.VMEM((SLOTS, ZS - 1, *piece[2:]), bf16),
            pltpu.VMEM((SLOTS, ZS - 1, *piece[2:]), bf16),
            pltpu.VMEM((SLOTS, *piece[2:]), bf16),
            pair,
            pair,
            pair,
            triple,
            triple,
            pair,
            pltpu.SemaphoreType.DMA((SLOTS,)),
            pltpu.SemaphoreType.DMA,
            pltpu.SemaphoreType.REGULAR((6,)),
        ]
    args = (h, dy, wg, wu, wd) + ((g1,) if reduce else ())
    return pl.pallas_call(
        lambda *refs: bwd_kernel(reduce, *refs),
        out_shape=tuple(outs),
        in_specs=[anywhere] * len(args),
        out_specs=(anywhere,) * len(outs),
        scratch_shapes=scratch,
        compiler_params=pltpu.CompilerParams(
            vmem_limit_bytes=VMEM_LIMIT, **(dict(collective_id=1, has_side_effects=True) if reduce else {})
        ),
        cost_estimate=pl.CostEstimate(flops=16 * T * D * F, bytes_accessed=30_000_000, transcendentals=0),
        name="backward_reduce" if reduce else "backward",
    )(*args)


def solution(mesh):
    def step(x, dy, *weights):
        def fetched(l):
            wg, wu, wd = [lax.all_gather(w[l], "s", axis=0, tiled=True) for w in weights]
            cols = [w.reshape(D, 4, J, QL).transpose(2, 0, 1, 3).reshape(J, D, FC) for w in (wg, wu)]
            return (*cols, wd.reshape(4, J, QL, D).transpose(1, 0, 2, 3).reshape(J, FC, D))

        w0, w1 = fetched(0), fetched(1)
        h0, dy = x.reshape(NB, TB, D), dy.reshape(NB, TB, D)
        h1 = forward(h0, *w0)
        dh1, g1 = backward(h1, dy, *w1)
        dx, _, total = backward(h0, dh1, *w0, g1)
        total = total.reshape(2, J, 3, 2, 4, HR, QL)[::-1]
        cols = [total[:, :, m].transpose(0, 2, 4, 3, 1, 5).reshape(2, 2 * HR, F) for m in range(2)]
        down = total[:, :, 2].transpose(0, 1, 5, 3, 2, 4).reshape(2, F // 4, D)
        return dx.reshape(1, T, D), *cols, down

    states, cut = P(("rep", "r", "s"), None, None), P(None, "s", None)
    return jax.shard_map(
        step,
        mesh=mesh,
        in_specs=(states, states) + (cut,) * 3,
        out_specs=(states,) + (P("rep", "s", None),) * 3,
        check_vma=False,
    )
```

```python
import jax
import jax.numpy as jnp
from jax import lax
from jax.experimental import pallas as pl
from jax.experimental.pallas import tpu as pltpu
from jax.sharding import PartitionSpec as P

T, D, F = 4096, 640, 2048
TB, FC = 512, 512
NB, J = T // TB, F // FC
STEPS = NB * J
XS, CS, YS, ZS = 2, 2, 2, 4
HR, DR, QL = D // 8, FC // 8, FC // 4
GATE_UP, DOWN = (2, J, 4, 2, HR, FC), (J, 4, 2, DR, D)
SLOTS = 6
TICKS = 46
VMEM_LIMIT = 67_000_000
bf16, f32 = jnp.bfloat16, jnp.float32
NT = (((1,), (1,)), ((), ()))
MESH = pl.DeviceIdType.MESH


def dot(a, b):
    return jnp.dot(a, b, preferred_element_type=f32)


def dot_nt(a, b):
    return lax.dot_general(a, b, NT, preferred_element_type=f32)


def scale_of(wide):
    return lax.rsqrt(jnp.mean(wide * wide, -1, keepdims=True) + 1e-6)


class Gather:
    def __init__(self, args, outs, w_v, own, lsem, osem, isem, psem, xsem, rsem, esem):
        self.__dict__.update({k: v for k, v in locals().items() if k != "self"})
        r, s = lax.axis_index("r"), lax.axis_index("s")
        self.r, self.s, self.y, self.z, x, c = r, s, r // ZS, r % ZS, s // CS, s % CS
        self.far = (1 - x) * CS + c
        self.partner = {"s": x * CS + 1 - c}
        self.xpeer = {"s": self.far}
        self.ypeer = {"r": (1 - self.y) * ZS + self.z}
        self.zpeers = [{"r": self.y * ZS + (self.z + d) % ZS} for d in range(1, ZS)]

    def enter(self):
        barrier = pltpu.get_barrier_semaphore()
        peers = [self.partner, self.xpeer, self.ypeer, *self.zpeers]
        for peer in peers:
            pl.semaphore_signal(barrier, inc=1, device_id=peer, device_id_type=MESH)
        pl.semaphore_wait(barrier, len(peers))

    def remote(self, src, dst, sems, peer):
        return pltpu.make_async_remote_copy(src, dst, sems.at[0], sems.at[1], device_id=peer, device_id_type=MESH)

    def mine(self, layer):
        wg, wu, wd = self.args
        copies, n = [], 0
        for j in range(J):
            gu, down = (self.w_v[0].at[:, j, self.s], self.w_v[1].at[j, self.s]) if layer == 0 else (self.own[0].at[:, j], self.own[1].at[j])
            for m, w in enumerate((wg, wu)):
                for q in range(4):
                    for h in range(2):
                        part = w.at[layer, pl.ds(h * HR, HR), pl.ds(q * FC + j * QL, QL)]
                        copies.append(pltpu.make_async_copy(part, gu.at[m, h, :, pl.ds(q * QL, QL)], self.lsem.at[layer, n]))
                        n += 1
            for h in range(2):
                part = wd.at[layer, pl.ds(j * QL + h * DR, DR), :]
                copies.append(pltpu.make_async_copy(part, down.at[h], self.lsem.at[layer, n]))
                n += 1
        return copies

    def hand(self, kind, j):
        s = self.far if kind == 2 else self.s
        peer = self.xpeer if kind == 1 else self.partner
        return [
            self.remote(ref, ref, self.psem.at[kind, j, n], peer)
            for n, ref in enumerate((self.w_v[0].at[:, j, s], self.w_v[1].at[j, s]))
        ]

    def save0(self, j):
        return [pltpu.make_async_copy(self.w_v[0].at[:, j], self.outs[0].at[:, j], self.osem.at[j, 0]), pltpu.make_async_copy(self.w_v[1].at[j], self.outs[1].at[j], self.osem.at[j, 1])]

    def own1(self):
        gu, down = self.outs[2].at[:, :, self.s], self.outs[3].at[:, self.s]
        return [
            pltpu.make_async_copy(self.own[0], gu, self.isem.at[0]),
            pltpu.make_async_copy(self.own[1], down, self.isem.at[1]),
            self.remote(self.own[0], gu, self.esem.at[0], self.partner),
            self.remote(self.own[1], down, self.esem.at[1], self.partner),
        ]

    def x1(self):
        j, h = self.r // 2, self.r % 2
        return [
            self.remote(self.own[0].at[:, j, h], self.outs[2].at[:, j, self.s, h], self.xsem.at[0], self.xpeer),
            self.remote(self.own[1].at[j, h], self.outs[3].at[j, self.s, h], self.xsem.at[1], self.xpeer),
        ]

    def z1(self):
        j, h = self.r // 2, self.r % 2
        refs = (self.outs[2].at[:, j, self.far, h], self.outs[3].at[j, self.far, h])
        return [self.remote(ref, ref, self.rsem.at[i, n], peer) for i, peer in enumerate(self.zpeers) for n, ref in enumerate(refs)]

    def part(self, y, sems, peer):
        refs = (self.outs[2].at[:, pl.ds(2 * y, 2), self.far], self.outs[3].at[pl.ds(2 * y, 2), self.far])
        return [self.remote(ref, ref, self.esem.at[sems + n], peer) for n, ref in enumerate(refs)]

    def y1(self):
        return self.part(self.y, 2, self.ypeer)

    def p1(self):
        return self.part(self.y, 4, self.partner)

    def p2(self):
        return self.part(1 - self.y, 6, self.partner)

    def tick(self, i):
        @pl.when(i == 2)
        def _():
            wait(self.x1())
            start(self.z1())

        @pl.when(i == 18)
        def _():
            wait(self.z1())
            start(self.y1())
            start(self.p1())

        for j in range(1, J):

            @pl.when(i == NB * j - 2)
            def _():
                wait(self.hand(1, j))
                start(self.hand(2, j))

    def arrive(self, j):
        wait(self.hand(0, j))
        wait(self.hand(2, j))
        start(self.save0(j))

    def leave(self):
        for j in range(J):
            wait(self.save0(j))
        wait(self.own1())
        wait(self.y1())
        start(self.p2())
        wait(self.p1())
        wait(self.p2())


def start(copies):
    for copy in copies:
        copy.start()


def wait(copies):
    for copy in copies:
        copy.wait()


def rows(ref, *index):
    got = ref[index]
    return got.reshape(-1, got.shape[-1])


def fwd_kernel(h_hbm, wg_hbm, wu_hbm, wd_hbm, o_hbm, *refs):
    outs, (h_v, a_v, yT_v, wgu_v, wd_v, wdT_v, s_v, owngu, ownd, hsem, *sems) = refs[:4], refs[4:]
    gather = Gather((wg_hbm, wu_hbm, wd_hbm), outs, (wgu_v, wd_v), (owngu, ownd), *sems)
    load = pltpu.make_async_copy(h_hbm, h_v, hsem)
    mine = gather.mine(0)
    start(mine)
    start(gather.mine(1))
    load.start()
    gather.enter()
    wait(mine)
    start(gather.hand(1, 0))
    start(gather.hand(0, 0))
    wait(gather.mine(1))
    start(gather.x1())
    for j in range(1, J):
        start(gather.hand(1, j))
        start(gather.hand(0, j))
    start(gather.own1())
    yT_v[...] = jnp.zeros_like(yT_v)
    s_v[1] = jnp.zeros_like(s_v[1])
    wdT_v[...] = jnp.zeros_like(wdT_v)
    load.wait()

    @pl.loop(0, NB)
    def _(t):
        wide = h_v[t].astype(f32)
        a_v[t] = (wide * scale_of(wide)).astype(bf16)

    wait(gather.hand(1, 0))
    start(gather.hand(2, 0))

    def front(j, t):
        return dot(a_v[t], rows(wgu_v, 0, j)), dot(a_v[t], rows(wgu_v, 1, j))

    def mid(gate, up):
        return (gate * jax.nn.sigmoid(gate) * up).astype(bf16)

    def back(j, t, act):
        yT_v[t] += dot_nt(wdT_v[j], act)

    @pl.loop(0, STEPS // 2)
    def _(pair):
        i = 2 * pair
        for j in range(J):

            @pl.when(i == NB * j)
            def _():
                gather.arrive(j)

        @pl.when(i % NB == 0)
        def _():
            wdT_v[i // NB] = rows(wd_v, i // NB).T

        before = jnp.maximum(i - 1, 0)
        first = front(i // NB, i % NB)
        back(before // NB, before % NB, s_v[1])
        s_v[0] = mid(*first)
        second = front((i + 1) // NB, (i + 1) % NB)
        back(i // NB, i % NB, s_v[0])
        s_v[1] = mid(*second)
        gather.tick(i)

    back(J - 1, NB - 1, s_v[1])

    @pl.loop(0, NB)
    def _(t):
        h_v[t] = h_v[t] + yT_v[t].astype(bf16).T

    copy = pltpu.make_async_copy(h_v, o_hbm, hsem)
    copy.start()
    gather.leave()
    copy.wait()


def forward(h, *weights):
    anywhere = pl.BlockSpec(memory_space=pl.ANY)
    shapes = [jax.ShapeDtypeStruct(s, bf16) for s in (GATE_UP, DOWN)]
    dma = pltpu.SemaphoreType.DMA
    return pl.pallas_call(
        fwd_kernel,
        out_shape=(jax.ShapeDtypeStruct((NB, TB, D), bf16), *shapes, *shapes),
        in_specs=[anywhere] * 4,
        out_specs=(anywhere,) * 5,
        scratch_shapes=[
            pltpu.VMEM((NB, TB, D), bf16),
            pltpu.VMEM((NB, TB, D), bf16),
            pltpu.VMEM((NB, D, TB), f32),
            pltpu.VMEM(GATE_UP, bf16),
            pltpu.VMEM(DOWN, bf16),
            pltpu.VMEM((J, D, FC), bf16),
            pltpu.VMEM((2, TB, FC), bf16),
            pltpu.VMEM((2, J, 2, HR, FC), bf16),
            pltpu.VMEM((J, 2, DR, D), bf16),
            dma,
            dma((2, 18 * J)),
            dma((J, 2)),
            dma((2,)),
            dma((3, J, 2, 2)),
            dma((2, 2)),
            dma((ZS - 1, 2, 2)),
            dma((8, 2)),
        ],
        compiler_params=pltpu.CompilerParams(vmem_limit_bytes=VMEM_LIMIT, collective_id=0, has_side_effects=True),
        cost_estimate=pl.CostEstimate(flops=6 * T * D * F, bytes_accessed=20_000_000, transcendentals=0),
        name="forward_gather",
    )(h, *weights)


class Reduction:
    def __init__(self, g1_hbm, g0_hbm, out_hbm, gbuf, drecv, xs, xrecv, ys, yrecv, keep, zs, zrecv, fq, dsem, xsem, ysem, zsem, fsem, asem, lsem, psem, near):
        self.__dict__.update({k: v for k, v in locals().items() if k != "self"})
        r, s = lax.axis_index("r"), lax.axis_index("s")
        self.y, self.z, self.x, self.c = r // ZS, r % ZS, s // CS, s % CS
        self.partner = {"s": self.x * CS + 1 - self.c}
        self.xpeer = {"s": (1 - self.x) * CS + self.c}
        self.ypeer = {"r": (1 - self.y) * ZS + self.z}
        self.zpeers = [{"r": self.y * ZS + (self.z + d) % ZS} for d in range(1, ZS)]
        self.peers = [self.partner, self.xpeer, self.ypeer, *self.zpeers]

    def enter(self):
        barrier = pltpu.get_barrier_semaphore()
        for peer in self.peers:
            pl.semaphore_signal(barrier, inc=1, device_id=peer, device_id_type=MESH)
        pl.semaphore_wait(barrier, len(self.peers))

    def load(self, g):
        return pltpu.make_async_copy(self.g1_hbm.at[g], self.gbuf.at[g % 2], self.psem)

    def load0(self, g):
        return pltpu.make_async_copy(self.g0_hbm.at[g - J], self.gbuf.at[g % 2], self.psem)

    def at(self, k):
        block = k // 4
        return (k >= 0) & (k % 4 < 3) & (block != 6) & (block < 9), block - jnp.where(block > 6, 1, 0), k % 4

    def remote(self, src, dst, sems, peer):
        return pltpu.make_async_remote_copy(src, dst, sems.at[0], sems.at[1], device_id=peer, device_id_type=MESH)

    def dcopy(self, b, m, slot):
        return self.remote(self.gbuf.at[b, m, 1 - self.c], self.drecv.at[slot], self.dsem.at[slot], self.partner)

    def xcopy(self, slot):
        return self.remote(self.xs.at[slot], self.xrecv.at[slot], self.xsem.at[slot], self.xpeer)

    def ycopy(self, slot):
        return self.remote(self.ys.at[slot], self.yrecv.at[slot], self.ysem.at[slot], self.ypeer)

    def zcopies(self, slot):
        return [self.remote(self.zs.at[slot, i], self.zrecv.at[slot, i], self.zsem.at[slot, i], peer) for i, peer in enumerate(self.zpeers)]

    def fcopies(self, g, m, slot):
        place = self.out_hbm.at[g, m, self.y, self.z]
        return [self.remote(self.fq.at[slot], place, self.fsem.at[slot, i], peer) for i, peer in enumerate(self.zpeers)] + [
            pltpu.make_async_copy(self.fq.at[slot], place, self.lsem.at[slot])
        ]

    def acopy(self, g, m, slot):
        half = self.out_hbm.at[g, m, self.y]
        return self.remote(half, half, self.asem.at[slot], self.ypeer)

    def stage(self, k, delay, body):
        valid, g, m = self.at(k - delay)

        @pl.when(valid)
        def _():
            body(g, m, (k - delay) % SLOTS)

    def tick(self, k):
        x, c, y, z = self.x, self.c, self.y, self.z
        gbuf, drecv, xrecv, keep = self.gbuf, self.drecv, self.xrecv, self.keep

        @pl.when(k >= 2)
        def _():
            for i in range(len(self.peers)):
                pl.semaphore_wait(self.near.at[i], 1)

        ahead = k + 2
        block = ahead // 4
        turn = (ahead % 4 == 0) & (k >= 0)

        @pl.when(turn & (block < J))
        def _():
            self.load(block).start()

        @pl.when(turn & (block >= J) & (block < 8) & (block != 6))
        def _():
            self.load0(block - jnp.where(block > 6, 1, 0)).start()

        def end(g, m, slot):
            self.acopy(g, m, slot).wait()

        def gather_y(g, m, slot):
            for copy in self.fcopies(g, m, slot):
                copy.wait()
            self.acopy(g, m, slot).start()

        def finish(g, m, slot):
            for copy in self.zcopies(slot):
                copy.wait()
            total = keep[slot, z]
            for i in range(ZS - 1):
                total += self.zrecv[slot, i].astype(f32)
            self.fq[slot] = total.astype(bf16)
            for copy in self.fcopies(g, m, slot):
                copy.start()

        def to_z(g, m, slot):
            self.ycopy(slot).wait()
            keep[slot] += self.yrecv[slot].astype(f32)
            for i in range(ZS - 1):
                self.zs[slot, i] = keep[slot, (z + i + 1) % ZS].astype(bf16)
            for copy in self.zcopies(slot):
                copy.start()

        def to_y(g, m, slot):
            self.xcopy(slot).wait()

            def total(half):
                return gbuf[g % 2, m, c, x, half].astype(f32) + drecv[slot, x, half].astype(f32) + xrecv[slot, half].astype(f32)

            self.ys[slot] = total(1 - y).astype(bf16)
            self.ycopy(slot).start()
            keep[slot] = total(y)

        def to_x(g, m, slot):
            self.dcopy(g % 2, m, slot).wait()
            self.xs[slot] = (gbuf[g % 2, m, c, 1 - x].astype(f32) + drecv[slot, 1 - x].astype(f32)).astype(bf16)
            self.xcopy(slot).start()

        def to_partner(g, m, slot):
            @pl.when((m == 0) & (g < J))
            def _():
                self.load(g).wait()

            @pl.when((m == 0) & (g >= J) & (g < 2 * J - 1))
            def _():
                self.load0(g).wait()

            self.dcopy(g % 2, m, slot).start()

        self.stage(k, 11, end)
        self.stage(k, 9, gather_y)
        self.stage(k, 7, finish)
        self.stage(k, 5, to_z)
        self.stage(k, 3, to_y)
        self.stage(k, 1, to_x)
        self.stage(k, 0, to_partner)

        @pl.when(k < TICKS - 2)
        def _():
            for i, peer in enumerate(self.peers):
                pl.semaphore_signal(self.near.at[i], inc=1, device_id=peer, device_id_type=MESH)


def bwd_kernel(reduce, *refs):
    h_hbm, dy_hbm, wgu_hbm, wd_hbm, *refs = refs
    g1_hbm, dh_hbm, g_hbm, *refs = refs if reduce else (None, *refs)
    out_hbm, *refs = refs if reduce else (None, *refs)
    dy_v, a_v, aT_v, dyT_v, daT_v, wgu_v, wd_v, acc_v, gb_v, s_v, sem, gsem, hsem, *refs = refs
    copies = [
        pltpu.make_async_copy(src, dst, sem.at[i])
        for i, (src, dst) in enumerate([(h_hbm, a_v), (dy_hbm, dy_v), (wgu_hbm, wgu_v), (wd_hbm, wd_v)])
    ]
    for copy in copies:
        copy.start()
    red = None
    if reduce:
        red = Reduction(g1_hbm, g_hbm, out_hbm, *refs)
        red.load(0).start()
        red.enter()
    acc_v[...] = jnp.zeros_like(acc_v)
    daT_v[...] = jnp.zeros_like(daT_v)
    s_v[1] = jnp.zeros_like(s_v[1])
    copies[0].wait()
    copies[1].wait()

    @pl.loop(0, NB)
    def _(t):
        wide = a_v[t].astype(f32)
        a = (wide * scale_of(wide)).astype(bf16)
        a_v[t] = a
        aT_v[t] = a.T
        dyT_v[t] = dy_v[t].T

    for copy in copies[2:]:
        copy.wait()

    def front(j, t):
        return dot(a_v[t], rows(wgu_v, 0, j)), dot(a_v[t], rows(wgu_v, 1, j)), dot_nt(dy_v[t], rows(wd_v, j))

    def mid(slot, gate, up, dact):
        dact = dact.astype(bf16).astype(f32)
        sg = jax.nn.sigmoid(gate)
        s = gate * sg
        s_v[slot, 0] = (s * up).astype(bf16)
        s_v[slot, 1] = (dact * up * (sg + s * (1.0 - sg))).astype(bf16)
        s_v[slot, 2] = (dact * s).astype(bf16)

    def back(j, t, slot):
        act, dgate, dup = s_v[slot, 0], s_v[slot, 1], s_v[slot, 2]
        daT_v[t] += dot_nt(rows(wgu_v, 0, j), dgate) + dot_nt(rows(wgu_v, 1, j), dup)
        acc_v[0] += dot(aT_v[t], dgate)
        acc_v[1] += dot(aT_v[t], dup)
        acc_v[2] += dot(dyT_v[t], act)

    def flush(dst):
        for x in range(XS):
            for c in range(CS):
                n = x * CS + c
                for h in range(2):
                    for q in range(4):
                        rows = slice(n * 2 * HR + h * HR, n * 2 * HR + (h + 1) * HR)
                        for m in range(2):
                            dst[m, c, x, h, q] = acc_v[m, rows, q * QL : (q + 1) * QL].astype(bf16)
                        rows = slice(q * 2 * HR + h * HR, q * 2 * HR + (h + 1) * HR)
                        dst[2, c, x, h, q] = acc_v[2, rows, n * QL : (n + 1) * QL].astype(bf16)

    def put(j):
        return pltpu.make_async_copy(gb_v, g_hbm.at[j], gsem)

    @pl.loop(0, STEPS // 2)
    def _(pair):
        i = 2 * pair
        before = jnp.maximum(i - 1, 0)
        first = front(i // NB, i % NB)
        back(before // NB, before % NB, 1)
        mid(0, *first)

        @pl.when((i % NB == 0) & (pair > 0))
        def _():
            flush(gb_v)
            put(before // NB).start()
            acc_v[...] = jnp.zeros_like(acc_v)

        if reduce:
            red.tick(i)
        second = front((i + 1) // NB, (i + 1) % NB)
        back(i // NB, i % NB, 0)
        mid(1, *second)

        @pl.when((i % NB == 0) & (pair > 0))
        def _():
            put(before // NB).wait()

        if reduce:
            red.tick(i + 1)

    reload = pltpu.make_async_copy(h_hbm, a_v, hsem)
    reload.start()
    back(J - 1, NB - 1, 1)
    if reduce:
        flush(red.gbuf.at[1])
    else:
        flush(gb_v)
        put(J - 1).start()
    reload.wait()

    @pl.loop(0, NB)
    def _(t):
        if reduce:
            red.tick(STEPS + t)
        da = daT_v[t].astype(bf16).T.astype(f32)
        wide = a_v[t].astype(f32)
        scale = scale_of(wide)
        mean = jnp.mean(da * wide, -1, keepdims=True)
        dy_v[t] = dy_v[t] + (da * scale - wide * (scale * scale * scale * mean)).astype(bf16)

    copy = pltpu.make_async_copy(dy_v, dh_hbm, hsem)
    copy.start()
    if reduce:

        @pl.loop(STEPS + NB, TICKS)
        def _(k):
            red.tick(k)

    else:
        put(J - 1).wait()
    copy.wait()


def backward(h, dy, wgu, wd, g1=None):
    reduce = g1 is not None
    anywhere = pl.BlockSpec(memory_space=pl.ANY)
    tokens, turned, grads = (NB, TB, D), (NB, D, TB), (J, 3, CS, XS, 2, 4, HR, QL)
    outs = [jax.ShapeDtypeStruct(tokens, bf16), jax.ShapeDtypeStruct(grads, bf16)]
    scratch = [
        pltpu.VMEM(tokens, bf16),
        pltpu.VMEM(tokens, bf16),
        pltpu.VMEM(turned, bf16),
        pltpu.VMEM(turned, bf16),
        pltpu.VMEM(turned, f32),
        pltpu.VMEM(GATE_UP, bf16),
        pltpu.VMEM(DOWN, bf16),
        pltpu.VMEM((3, D, FC), f32),
        pltpu.VMEM(grads[1:], bf16),
        pltpu.VMEM((2, 3, TB, FC), bf16),
        pltpu.SemaphoreType.DMA((4,)),
        pltpu.SemaphoreType.DMA,
        pltpu.SemaphoreType.DMA,
    ]
    if reduce:
        piece = (2, 4, HR, QL)
        outs.append(jax.ShapeDtypeStruct((2 * J, 3, *piece), bf16))
        pair = pltpu.SemaphoreType.DMA((SLOTS, 2))
        triple = pltpu.SemaphoreType.DMA((SLOTS, ZS - 1, 2))
        scratch += [
            pltpu.VMEM((2, *grads[1:]), bf16),
            pltpu.VMEM((SLOTS, XS, *piece), bf16),
            pltpu.VMEM((SLOTS, *piece), bf16),
            pltpu.VMEM((SLOTS, *piece), bf16),
            pltpu.VMEM((SLOTS, *piece[1:]), bf16),
            pltpu.VMEM((SLOTS, *piece[1:]), bf16),
            pltpu.VMEM((SLOTS, *piece[1:]), f32),
            pltpu.VMEM((SLOTS, ZS - 1, *piece[2:]), bf16),
            pltpu.VMEM((SLOTS, ZS - 1, *piece[2:]), bf16),
            pltpu.VMEM((SLOTS, *piece[2:]), bf16),
            pair,
            pair,
            pair,
            triple,
            triple,
            pair,
            pltpu.SemaphoreType.DMA((SLOTS,)),
            pltpu.SemaphoreType.DMA,
            pltpu.SemaphoreType.REGULAR((6,)),
        ]
    args = (h, dy, wgu, wd) + ((g1,) if reduce else ())
    return pl.pallas_call(
        lambda *refs: bwd_kernel(reduce, *refs),
        out_shape=tuple(outs),
        in_specs=[anywhere] * len(args),
        out_specs=(anywhere,) * len(outs),
        scratch_shapes=scratch,
        compiler_params=pltpu.CompilerParams(
            vmem_limit_bytes=VMEM_LIMIT, **(dict(collective_id=1, has_side_effects=True) if reduce else {})
        ),
        cost_estimate=pl.CostEstimate(flops=16 * T * D * F, bytes_accessed=30_000_000, transcendentals=0),
        name="backward_reduce" if reduce else "backward",
    )(*args)


def solution(mesh):
    def step(x, dy, *weights):
        h0, dy = x.reshape(NB, TB, D), dy.reshape(NB, TB, D)
        h1, gate_up0, down0, gate_up1, down1 = forward(h0, *weights)
        dh1, g1 = backward(h1, dy, gate_up1, down1)
        dx, _, total = backward(h0, dh1, gate_up0, down0, g1)
        total = total.reshape(2, J, 3, 2, 4, HR, QL)[::-1]
        cols = [total[:, :, m].transpose(0, 2, 4, 3, 1, 5).reshape(2, 2 * HR, F) for m in range(2)]
        down = total[:, :, 2].transpose(0, 1, 5, 3, 2, 4).reshape(2, F // 4, D)
        return dx.reshape(1, T, D), *cols, down

    states, cut = P(("rep", "r", "s"), None, None), P(None, "s", None)
    return jax.shard_map(
        step,
        mesh=mesh,
        in_specs=(states, states) + (cut,) * 3,
        out_specs=(states,) + (P("rep", "s", None),) * 3,
        check_vma=False,
    )
```

```python
import jax
import jax.numpy as jnp
from jax import lax
from jax.experimental import pallas as pl
from jax.experimental.pallas import tpu as pltpu
from jax.sharding import PartitionSpec as P

T, D, F = 4096, 640, 2048
TB, FC = 512, 512
NB, J = T // TB, F // FC
STEPS = NB * J
XS, CS, YS, ZS = 2, 2, 2, 4
HR, DR, QL = D // 8, FC // 8, FC // 4
GATE_UP, DOWN = (2, J, 4, 2, HR, FC), (J, 4, 2, DR, D)
SLOTS = 6
DEEP, AHEAD = 4, 2
VMEM_LIMIT = 67_000_000
bf16, f32 = jnp.bfloat16, jnp.float32
NT = (((1,), (1,)), ((), ()))
MESH = pl.DeviceIdType.MESH


def dot(a, b):
    return jnp.dot(a, b, preferred_element_type=f32)


def dot_nt(a, b):
    return lax.dot_general(a, b, NT, preferred_element_type=f32)


def scale_of(wide):
    return lax.rsqrt(jnp.mean(wide * wide, -1, keepdims=True) + 1e-6)


class Gather:
    def __init__(self, args, outs, w_v, own, lsem, osem, isem, psem, xsem, rsem, esem):
        self.__dict__.update({k: v for k, v in locals().items() if k != "self"})
        r, s = lax.axis_index("r"), lax.axis_index("s")
        self.r, self.s, self.y, self.z, x, c = r, s, r // ZS, r % ZS, s // CS, s % CS
        self.far = (1 - x) * CS + c
        self.partner = {"s": x * CS + 1 - c}
        self.xpeer = {"s": self.far}
        self.ypeer = {"r": (1 - self.y) * ZS + self.z}
        self.zpeers = [{"r": self.y * ZS + (self.z + d) % ZS} for d in range(1, ZS)]

    def enter(self):
        barrier = pltpu.get_barrier_semaphore()
        peers = [self.partner, self.xpeer, self.ypeer, *self.zpeers]
        for peer in peers:
            pl.semaphore_signal(barrier, inc=1, device_id=peer, device_id_type=MESH)
        pl.semaphore_wait(barrier, len(peers))

    def remote(self, src, dst, sems, peer):
        return pltpu.make_async_remote_copy(src, dst, sems.at[0], sems.at[1], device_id=peer, device_id_type=MESH)

    def mine(self, layer):
        wg, wu, wd = self.args
        copies, n = [], 0
        for j in range(J):
            gu, down = (self.w_v[0].at[:, j, self.s], self.w_v[1].at[j, self.s]) if layer == 0 else (self.own[0].at[:, j], self.own[1].at[j])
            for m, w in enumerate((wg, wu)):
                for q in range(4):
                    for h in range(2):
                        part = w.at[layer, pl.ds(h * HR, HR), pl.ds(q * FC + j * QL, QL)]
                        copies.append(pltpu.make_async_copy(part, gu.at[m, h, :, pl.ds(q * QL, QL)], self.lsem.at[layer, n]))
                        n += 1
            for h in range(2):
                part = wd.at[layer, pl.ds(j * QL + h * DR, DR), :]
                copies.append(pltpu.make_async_copy(part, down.at[h], self.lsem.at[layer, n]))
                n += 1
        return copies

    def hand(self, kind, j):
        s = self.far if kind == 2 else self.s
        peer = self.xpeer if kind == 1 else self.partner
        return [
            self.remote(ref, ref, self.psem.at[kind, j, n], peer)
            for n, ref in enumerate((self.w_v[0].at[:, j, s], self.w_v[1].at[j, s]))
        ]

    def save0(self, j):
        return [pltpu.make_async_copy(self.w_v[0].at[:, j], self.outs[0].at[:, j], self.osem.at[j, 0]), pltpu.make_async_copy(self.w_v[1].at[j], self.outs[1].at[j], self.osem.at[j, 1])]

    def own1(self):
        gu, down = self.outs[2].at[:, :, self.s], self.outs[3].at[:, self.s]
        return [
            pltpu.make_async_copy(self.own[0], gu, self.isem.at[0]),
            pltpu.make_async_copy(self.own[1], down, self.isem.at[1]),
            self.remote(self.own[0], gu, self.esem.at[0], self.partner),
            self.remote(self.own[1], down, self.esem.at[1], self.partner),
        ]

    def x1(self):
        j, h = self.r // 2, self.r % 2
        return [
            self.remote(self.own[0].at[:, j, h], self.outs[2].at[:, j, self.s, h], self.xsem.at[0], self.xpeer),
            self.remote(self.own[1].at[j, h], self.outs[3].at[j, self.s, h], self.xsem.at[1], self.xpeer),
        ]

    def z1(self):
        j, h = self.r // 2, self.r % 2
        refs = (self.outs[2].at[:, j, self.far, h], self.outs[3].at[j, self.far, h])
        return [self.remote(ref, ref, self.rsem.at[i, n], peer) for i, peer in enumerate(self.zpeers) for n, ref in enumerate(refs)]

    def part(self, y, sems, peer):
        refs = (self.outs[2].at[:, pl.ds(2 * y, 2), self.far], self.outs[3].at[pl.ds(2 * y, 2), self.far])
        return [self.remote(ref, ref, self.esem.at[sems + n], peer) for n, ref in enumerate(refs)]

    def y1(self):
        return self.part(self.y, 2, self.ypeer)

    def p1(self):
        return self.part(self.y, 4, self.partner)

    def p2(self):
        return self.part(1 - self.y, 6, self.partner)

    def tick(self, i):
        @pl.when(i == 2)
        def _():
            wait(self.x1())
            start(self.z1())

        @pl.when(i == 18)
        def _():
            wait(self.z1())
            start(self.y1())
            start(self.p1())

        for j in range(1, J):

            @pl.when(i == NB * j - 2)
            def _():
                wait(self.hand(1, j))
                start(self.hand(2, j))

    def arrive(self, j):
        wait(self.hand(0, j))
        wait(self.hand(2, j))
        start(self.save0(j))

    def leave(self):
        for j in range(J):
            wait(self.save0(j))
        wait(self.own1())
        wait(self.y1())
        start(self.p2())
        wait(self.p1())
        wait(self.p2())


def start(copies):
    for copy in copies:
        copy.start()


def wait(copies):
    for copy in copies:
        copy.wait()


def block(src, dst, t, sems):
    return pltpu.make_async_copy(src.at[t], dst.at[t], sems.at[t])


def rows(ref, *index):
    got = ref[index]
    return got.reshape(-1, got.shape[-1])


def fwd_kernel(h_hbm, wg_hbm, wu_hbm, wd_hbm, o_hbm, *refs):
    outs, gu_hbm, (h_v, a_v, yT_v, wgu_v, wd_v, wdT_v, s_v, gu_v, owngu, ownd, hsem, gsem, *sems) = refs[:4], refs[4], refs[5:]
    gather = Gather((wg_hbm, wu_hbm, wd_hbm), outs, (wgu_v, wd_v), (owngu, ownd), *sems)
    mine = gather.mine(0)
    start(mine)
    start(gather.mine(1))
    start([block(h_hbm, h_v, t, hsem) for t in range(NB)])
    gather.enter()
    wait(mine)
    start(gather.hand(1, 0))
    start(gather.hand(0, 0))
    wait(gather.mine(1))
    start(gather.x1())
    for j in range(1, J):
        start(gather.hand(1, j))
        start(gather.hand(0, j))
    start(gather.own1())
    yT_v[...] = jnp.zeros_like(yT_v)
    s_v[1] = jnp.zeros_like(s_v[1])
    wdT_v[...] = jnp.zeros_like(wdT_v)

    @pl.loop(0, NB)
    def _(t):
        block(h_hbm, h_v, t, hsem).wait()
        wide = h_v[t].astype(f32)
        a_v[t] = (wide * scale_of(wide)).astype(bf16)

    wait(gather.hand(1, 0))
    start(gather.hand(2, 0))

    def front(j, t):
        return dot(a_v[t], rows(wgu_v, 0, j)), dot(a_v[t], rows(wgu_v, 1, j))

    def mid(i, slot, gate, up):
        gu_v[i % DEEP, 0] = gate
        gu_v[i % DEEP, 1] = up
        s_v[slot] = (gate * jax.nn.sigmoid(gate) * up).astype(bf16)

    def save(i):
        return pltpu.make_async_copy(gu_v.at[i % DEEP], gu_hbm.at[i], gsem.at[i % DEEP])

    def back(j, t, act):
        yT_v[t] += dot_nt(wdT_v[j], act)

    @pl.loop(0, STEPS // 2)
    def _(pair):
        i = 2 * pair
        for j in range(J):

            @pl.when(i == NB * j)
            def _():
                gather.arrive(j)

        @pl.when(i % NB == 0)
        def _():
            wdT_v[i // NB] = rows(wd_v, i // NB).T

        @pl.when(i >= DEEP)
        def _():
            wait([save(i - DEEP), save(i + 1 - DEEP)])

        before = jnp.maximum(i - 1, 0)
        first = front(i // NB, i % NB)
        back(before // NB, before % NB, s_v[1])
        mid(i, 0, *first)
        second = front((i + 1) // NB, (i + 1) % NB)
        back(i // NB, i % NB, s_v[0])
        mid(i + 1, 1, *second)
        start([save(i), save(i + 1)])
        gather.tick(i)

    back(J - 1, NB - 1, s_v[1])

    @pl.loop(0, NB)
    def _(t):
        h_v[t] = h_v[t] + yT_v[t].astype(bf16).T
        block(h_v, o_hbm, t, hsem).start()

    gather.leave()
    wait([block(h_v, o_hbm, t, hsem) for t in range(NB)])
    wait([save(i) for i in range(STEPS - DEEP, STEPS)])


def forward(h, *weights):
    anywhere = pl.BlockSpec(memory_space=pl.ANY)
    shapes = [jax.ShapeDtypeStruct(s, bf16) for s in (GATE_UP, DOWN)]
    dma = pltpu.SemaphoreType.DMA
    return pl.pallas_call(
        fwd_kernel,
        out_shape=(jax.ShapeDtypeStruct((NB, TB, D), bf16), *shapes, *shapes, jax.ShapeDtypeStruct((STEPS, 2, TB, FC), f32)),
        in_specs=[anywhere] * 4,
        out_specs=(anywhere,) * 6,
        scratch_shapes=[
            pltpu.VMEM((NB, TB, D), bf16),
            pltpu.VMEM((NB, TB, D), bf16),
            pltpu.VMEM((NB, D, TB), f32),
            pltpu.VMEM(GATE_UP, bf16),
            pltpu.VMEM(DOWN, bf16),
            pltpu.VMEM((J, D, FC), bf16),
            pltpu.VMEM((2, TB, FC), bf16),
            pltpu.VMEM((DEEP, 2, TB, FC), f32),
            pltpu.VMEM((2, J, 2, HR, FC), bf16),
            pltpu.VMEM((J, 2, DR, D), bf16),
            dma((NB,)),
            dma((DEEP,)),
            dma((2, 18 * J)),
            dma((J, 2)),
            dma((2,)),
            dma((3, J, 2, 2)),
            dma((2, 2)),
            dma((ZS - 1, 2, 2)),
            dma((8, 2)),
        ],
        compiler_params=pltpu.CompilerParams(vmem_limit_bytes=VMEM_LIMIT, collective_id=0, has_side_effects=True),
        cost_estimate=pl.CostEstimate(flops=6 * T * D * F, bytes_accessed=20_000_000, transcendentals=0),
        name="forward_gather",
    )(h, *weights)


class Reduction:
    def __init__(self, groups, spread, delays, out_hbm, gbuf, drecv, xs, xrecv, ys, yrecv, keep, zs, zrecv, fq, dsem, xsem, ysem, zsem, fsem, asem, lsem, near):
        self.__dict__.update({k: v for k, v in locals().items() if k != "self"})
        r, s = lax.axis_index("r"), lax.axis_index("s")
        self.y, self.z, self.x, self.c = r // ZS, r % ZS, s // CS, s % CS
        self.partner = {"s": self.x * CS + 1 - self.c}
        self.xpeer = {"s": (1 - self.x) * CS + self.c}
        self.ypeer = {"r": (1 - self.y) * ZS + self.z}
        self.zpeers = [{"r": self.y * ZS + (self.z + d) % ZS} for d in range(1, ZS)]
        self.peers = [self.partner, self.xpeer, self.ypeer, *self.zpeers]

    def enter(self):
        barrier = pltpu.get_barrier_semaphore()
        for peer in self.peers:
            pl.semaphore_signal(barrier, inc=1, device_id=peer, device_id_type=MESH)
        pl.semaphore_wait(barrier, len(self.peers))

    def at(self, k):
        return (k >= 0) & (k % 8 < 3 * self.spread) & (k % self.spread == 0) & (k < 8 * self.groups), k // 8, k % 8 // self.spread

    def remote(self, src, dst, sems, peer):
        return pltpu.make_async_remote_copy(src, dst, sems.at[0], sems.at[1], device_id=peer, device_id_type=MESH)

    def dcopy(self, b, m, slot):
        return self.remote(self.gbuf.at[b, m, 1 - self.c], self.drecv.at[slot], self.dsem.at[slot], self.partner)

    def xcopy(self, slot):
        return self.remote(self.xs.at[slot], self.xrecv.at[slot], self.xsem.at[slot], self.xpeer)

    def ycopy(self, slot):
        return self.remote(self.ys.at[slot], self.yrecv.at[slot], self.ysem.at[slot], self.ypeer)

    def zcopies(self, slot):
        return [self.remote(self.zs.at[slot, i], self.zrecv.at[slot, i], self.zsem.at[slot, i], peer) for i, peer in enumerate(self.zpeers)]

    def fcopies(self, g, m, slot):
        place = self.out_hbm.at[g, m, self.y, self.z]
        return [self.remote(self.fq.at[slot], place, self.fsem.at[slot, i], peer) for i, peer in enumerate(self.zpeers)] + [
            pltpu.make_async_copy(self.fq.at[slot], place, self.lsem.at[slot])
        ]

    def acopy(self, g, m, slot):
        half = self.out_hbm.at[g, m, self.y]
        return self.remote(half, half, self.asem.at[slot], self.ypeer)

    def stage(self, k, delay, body):
        valid, g, m = self.at(k - delay)

        @pl.when(valid)
        def _():
            body(g, m, g % 2 * 3 + m)

    def tick(self, k):
        x, c, y, z = self.x, self.c, self.y, self.z
        gbuf, drecv, xrecv, keep = self.gbuf, self.drecv, self.xrecv, self.keep

        @pl.when((k % 8 == 0) & (k >= 16) & (k < 8 * self.groups))
        def _():
            for i in range(len(self.peers)):
                pl.semaphore_wait(self.near.at[i], 1)

        def end(g, m, slot):
            self.acopy(g, m, slot).wait()

        def gather_y(g, m, slot):
            for copy in self.fcopies(g, m, slot):
                copy.wait()
            self.acopy(g, m, slot).start()

        def finish(g, m, slot):
            for copy in self.zcopies(slot):
                copy.wait()
            total = keep[slot, z]
            for i in range(ZS - 1):
                total += self.zrecv[slot, i].astype(f32)
            self.fq[slot] = total.astype(bf16)
            for copy in self.fcopies(g, m, slot):
                copy.start()

        def to_z(g, m, slot):
            self.ycopy(slot).wait()
            keep[slot] += self.yrecv[slot].astype(f32)
            for i in range(ZS - 1):
                self.zs[slot, i] = keep[slot, (z + i + 1) % ZS].astype(bf16)
            for copy in self.zcopies(slot):
                copy.start()

        def to_y(g, m, slot):
            self.xcopy(slot).wait()

            def total(half):
                return gbuf[g % self.spread, m, c, x, half].astype(f32) + drecv[slot, x, half].astype(f32) + xrecv[slot, half].astype(f32)

            self.ys[slot] = total(1 - y).astype(bf16)
            self.ycopy(slot).start()
            keep[slot] = total(y)

        def to_x(g, m, slot):
            self.dcopy(g % self.spread, m, slot).wait()
            self.xs[slot] = (gbuf[g % self.spread, m, c, 1 - x].astype(f32) + drecv[slot, 1 - x].astype(f32)).astype(bf16)
            self.xcopy(slot).start()

        def to_partner(g, m, slot):
            self.dcopy(g % self.spread, m, slot).start()

        for delay, body in zip(self.delays, (end, gather_y, finish, to_z, to_y, to_x, to_partner), strict=True):
            self.stage(k, delay, body)
        done = 2 * self.spread + self.delays[2]

        @pl.when((k >= done) & ((k - done) % 8 == 0) & (k - done < 8 * (self.groups - 2)))
        def _():
            for i, peer in enumerate(self.peers):
                pl.semaphore_signal(self.near.at[i], inc=1, device_id=peer, device_id_type=MESH)


def bwd_kernel(last, *refs):
    h_hbm, dy_hbm, wgu_hbm, wd_hbm, *refs = refs
    if last:
        g_hbm, gu_hbm, dh_hbm, ds_hbm, out_hbm, *refs = refs
    else:
        dh_hbm, g_hbm, out_hbm, *refs = refs
    dy_v, h_v, aT_v, dyT_v, wgu_v, wd_v, acc_v, s_v, hsem, ysem, wsem, gsem, *refs = refs
    if last:
        daT_v, gu_v, ds_v, usem, dsem, esem, *refs = refs
    else:
        daT_v, a_v, *refs = refs
    plan = (J + 1, 2, (18, 14, 10, 6, 4, 1, 0)) if last else (J - 1, 1, (11, 9, 7, 5, 3, 1, 0))
    red = Reduction(*plan, out_hbm, *refs)

    def weights(j):
        return [pltpu.make_async_copy(wgu_hbm.at[:, j], wgu_v.at[:, j], wsem.at[j, 0]), pltpu.make_async_copy(wd_hbm.at[j], wd_v.at[j], wsem.at[j, 1])]

    def saved(i):
        return pltpu.make_async_copy(gu_hbm.at[i], gu_v.at[i % AHEAD], usem.at[i % AHEAD])

    def spill(i, slot):
        return pltpu.make_async_copy(s_v.at[slot, pl.ds(1, 2)], ds_hbm.at[i // NB, i % NB], dsem.at[slot])

    def fetch(t, slot):
        return pltpu.make_async_copy(ds_hbm.at[:, t], ds_v.at[slot], esem.at[slot])

    for t in range(NB):
        start([block(h_hbm, h_v, t, hsem), block(dy_hbm, dy_v, t, ysem)])
    for j in range(J):
        start(weights(j))
    if last:
        first_group = pltpu.make_async_copy(g_hbm, red.gbuf.at[0], gsem)
        start([first_group, *(saved(i) for i in range(AHEAD))])
    red.enter()
    acc_v[...] = jnp.zeros_like(acc_v)
    s_v[1] = jnp.zeros_like(s_v[1])
    if not last:
        daT_v[...] = jnp.zeros_like(daT_v)

    @pl.loop(0, NB)
    def _(t):
        wait([block(h_hbm, h_v, t, hsem), block(dy_hbm, dy_v, t, ysem)])
        wide = h_v[t].astype(f32)
        a = (wide * scale_of(wide)).astype(bf16)
        if not last:
            a_v[t] = a
        aT_v[t] = a.T
        dyT_v[t] = dy_v[t].T

    if last:
        first_group.wait()

    def front(j, t):
        dact = dot_nt(dy_v[t], rows(wd_v, j))
        if last:
            return (dact,)
        return dact, dot(a_v[t], rows(wgu_v, 0, j)), dot(a_v[t], rows(wgu_v, 1, j))

    def mid(i, slot, dact, gate=None, up=None):
        if last:
            gate, up = gu_v[i % AHEAD, 0], gu_v[i % AHEAD, 1]
        dact = dact.astype(bf16).astype(f32)
        sg = jax.nn.sigmoid(gate)
        s = gate * sg
        s_v[slot, 0] = (s * up).astype(bf16)
        s_v[slot, 1] = (dact * up * (sg + s * (1.0 - sg))).astype(bf16)
        s_v[slot, 2] = (dact * s).astype(bf16)
        if last:
            spill(i, slot).start()

            @pl.when(i + AHEAD < STEPS)
            def _():
                saved(i + AHEAD).start()

    def back(j, t, slot):
        act, dgate, dup = s_v[slot, 0], s_v[slot, 1], s_v[slot, 2]
        if not last:
            daT_v[t] += dot_nt(rows(wgu_v, 0, j), dgate) + dot_nt(rows(wgu_v, 1, j), dup)
        acc_v[0] += dot(aT_v[t], dgate)
        acc_v[1] += dot(aT_v[t], dup)
        acc_v[2] += dot(dyT_v[t], act)

    def flush(b):
        for x in range(XS):
            for c in range(CS):
                n = x * CS + c
                for h in range(2):
                    for q in range(4):
                        part = slice(n * 2 * HR + h * HR, n * 2 * HR + (h + 1) * HR)
                        for m in range(2):
                            red.gbuf[b, m, c, x, h, q] = acc_v[m, part, q * QL : (q + 1) * QL].astype(bf16)
                        part = slice(q * 2 * HR + h * HR, q * 2 * HR + (h + 1) * HR)
                        red.gbuf[b, 2, c, x, h, q] = acc_v[2, part, n * QL : (n + 1) * QL].astype(bf16)

    def tick(i):
        if last:
            red.tick(i)
        else:

            @pl.when(i >= NB)
            def _():
                red.tick(i - NB)

    def norm_back(t, da):
        da = da.astype(bf16).T.astype(f32)
        wide = h_v[t].astype(f32)
        scale = scale_of(wide)
        mean = jnp.mean(da * wide, -1, keepdims=True)
        dy_v[t] = dy_v[t] + (da * scale - wide * (scale * scale * scale * mean)).astype(bf16)
        block(dy_v, dh_hbm, t, hsem).start()

    @pl.loop(0, STEPS // 2)
    def _(pair):
        i = 2 * pair

        @pl.when(i % NB == 0)
        def _():
            wait(weights(i // NB))

        before = jnp.maximum(i - 1, 0)
        if last:

            @pl.when(pair > 0)
            def _():
                spill(i - 2, 0).wait()

            saved(i).wait()
        first = front(i // NB, i % NB)
        back(before // NB, before % NB, 1)
        mid(i, 0, *first)

        @pl.when((i % NB == 0) & (pair > 0))
        def _():
            flush(i // NB % red.spread)
            acc_v[...] = jnp.zeros_like(acc_v)

        tick(i)
        if last:

            @pl.when(pair > 0)
            def _():
                spill(i - 1, 1).wait()

            saved(i + 1).wait()
        second = front((i + 1) // NB, (i + 1) % NB)
        back(i // NB, i % NB, 0)
        mid(i + 1, 1, *second)
        tick(i + 1)

    if last:
        wait([spill(STEPS - 2, 0), spill(STEPS - 1, 1)])
        start([fetch(0, 0), fetch(1, 1)])
    back(J - 1, NB - 1, 1)
    flush(0)
    if last:

        @pl.loop(0, NB)
        def _(t):
            slot = t % 2
            fetch(t, slot).wait()
            red.tick(STEPS + 2 * t)

            def part(j):
                return dot_nt(rows(wgu_v, 0, j), ds_v[slot, j, 0]) + dot_nt(rows(wgu_v, 1, j), ds_v[slot, j, 1])

            daT_v[...] = part(0) + part(1)
            red.tick(STEPS + 2 * t + 1)
            norm_back(t, daT_v[...] + (part(2) + part(3)))

            @pl.when(t + 2 < NB)
            def _():
                fetch(t + 2, slot).start()

        @pl.loop(STEPS + 2 * NB, 8 * J + 4 + 19)
        def _(k):
            red.tick(k)

    else:
        put = pltpu.make_async_copy(red.gbuf.at[0], g_hbm, gsem)
        put.start()

        @pl.loop(0, NB)
        def _(t):
            tick(STEPS + t)
            norm_back(t, daT_v[t])

        put.wait()
    wait([block(dy_v, dh_hbm, t, hsem) for t in range(NB)])


def backward(h, dy, wgu, wd, *more):
    last = bool(more)
    anywhere = pl.BlockSpec(memory_space=pl.ANY)
    tokens, turned, grads, piece = (NB, TB, D), (NB, D, TB), (3, CS, XS, 2, 4, HR, QL), (2, 4, HR, QL)
    dma, vmem = pltpu.SemaphoreType.DMA, pltpu.VMEM
    total = jax.ShapeDtypeStruct((J + 1 if last else J - 1, 3, *piece), bf16)
    kept = jax.ShapeDtypeStruct((J, NB, 2, TB, FC) if last else grads, bf16)
    if last:
        own = [vmem((D, TB), f32), vmem((AHEAD, 2, TB, FC), f32), vmem((2, J, 2, TB, FC), bf16), dma((AHEAD,)), dma((2,)), dma((2,))]
    else:
        own = [vmem(turned, f32), vmem(tokens, bf16)]
    return pl.pallas_call(
        lambda *refs: bwd_kernel(last, *refs),
        out_shape=(jax.ShapeDtypeStruct(tokens, bf16), kept, total),
        in_specs=[anywhere] * (4 + len(more)),
        out_specs=(anywhere,) * 3,
        scratch_shapes=[
            vmem(tokens, bf16),
            vmem(tokens, bf16),
            vmem(turned, bf16),
            vmem(turned, bf16),
            vmem(GATE_UP, bf16),
            vmem(DOWN, bf16),
            vmem((3, D, FC), f32),
            vmem((2, 3, TB, FC), bf16),
            dma((NB,)),
            dma((NB,)),
            dma((J, 2)),
            dma,
            *own,
            vmem((2 if last else 1, *grads), bf16),
            vmem((SLOTS, XS, *piece), bf16),
            vmem((SLOTS, *piece), bf16),
            vmem((SLOTS, *piece), bf16),
            vmem((SLOTS, *piece[1:]), bf16),
            vmem((SLOTS, *piece[1:]), bf16),
            vmem((SLOTS, *piece[1:]), f32),
            vmem((SLOTS, ZS - 1, *piece[2:]), bf16),
            vmem((SLOTS, ZS - 1, *piece[2:]), bf16),
            vmem((SLOTS, *piece[2:]), bf16),
            dma((SLOTS, 2)),
            dma((SLOTS, 2)),
            dma((SLOTS, 2)),
            dma((SLOTS, ZS - 1, 2)),
            dma((SLOTS, ZS - 1, 2)),
            dma((SLOTS, 2)),
            dma((SLOTS,)),
            pltpu.SemaphoreType.REGULAR((6,)),
        ],
        compiler_params=pltpu.CompilerParams(vmem_limit_bytes=VMEM_LIMIT, collective_id=2 if last else 1, has_side_effects=True),
        cost_estimate=pl.CostEstimate(flops=(12 if last else 16) * T * D * F, bytes_accessed=30_000_000, transcendentals=0),
        name="backward_0" if last else "backward_1",
    )(h, dy, wgu, wd, *more)


def solution(mesh):
    def step(x, dy, *weights):
        h0, dy = x.reshape(NB, TB, D), dy.reshape(NB, TB, D)
        h1, gate_up0, down0, gate_up1, down1, saved = forward(h0, *weights)
        dh1, left, total1 = backward(h1, dy, gate_up1, down1)
        dx, _, total0 = backward(h0, dh1, gate_up0, down0, left, saved)
        total = jnp.concatenate([total0[1:], total1, total0[:1]]).reshape(2, J, 3, 2, 4, HR, QL)
        cols = [total[:, :, m].transpose(0, 2, 4, 3, 1, 5).reshape(2, 2 * HR, F) for m in range(2)]
        down = total[:, :, 2].transpose(0, 1, 5, 3, 2, 4).reshape(2, F // 4, D)
        return dx.reshape(1, T, D), *cols, down

    states, cut = P(("rep", "r", "s"), None, None), P(None, "s", None)
    return jax.shard_map(
        step,
        mesh=mesh,
        in_specs=(states, states) + (cut,) * 3,
        out_specs=(states,) + (P("rep", "s", None),) * 3,
        check_vma=False,
    )
```
